32 devices in a mesh: gx: 4 (over z), gy: 2 (over core), gz: 4 (over y, x).
Axes of the slice: x: 2, y: 2, z: 4, core: 2. Of those that a mesh axis runs over, the one named last changes fastest.
Arguments:
- pair: bfloat16 [128, 512, 512], P('gz', 'gx', 'gy'), may hold values from -6 to 6
- pair_mask: int32 [512, 512], P('gx', 'gy'), may hold values from 0 to 1, as said below
- input_gain: float32 [128], replicated, may hold values from 0.1 to 1.9
- input_weights: bfloat16 [4, 128, 128], replicated, may hold values from -0.5 to 0.5
- out_gate_weight: bfloat16 [128, 128], replicated, may hold values from -0.5 to 0.5
- hidden_gain: float32 [128], replicated, may hold values from 0.1 to 1.9
- out_weight: bfloat16 [128, 128], replicated, may hold values from -0.5 to 0.5
Outputs:
- update: bfloat16 [128, 512, 512], P('gz', 'gx', 'gy')
The draws below stay inside these ranges and needn't reach their ends.
Inputs may be any that keep to these rules, and one draw needn't show every extreme that they name: pair_mask[r, s] = m[r] * m[s] for a 0/1 residue mask m of the draw that is 0 for all r >= L, for one crop length L with 256 < L <= 512; residues below L may also be 0.
All inputs are finite; a program needn't handle non-finite values.
Results may differ from the reference program's by a relative error of at most 0.011.
Values may be sent and summed in bfloat16 or wider, within the bound.
No kernel may reach another device: no remote copies, remote signals or barrier semaphores. Data moves between devices by JAX's collectives and lax.ppermute only.
A program may use at most 64 MiB of HBM per device.

```python
import jax
import jax.numpy as jnp
from jax import lax

C = 128
CH = 128
N = 512


def draw_pair_mask(key, part):
    crop_length = jax.random.randint(jax.random.fold_in(key, 7), (), N // 2 + 1, N + 1)
    dropped = jax.random.randint(jax.random.fold_in(key, 11), (N,), 0, 16)
    inside = ((jnp.arange(N) < crop_length) & (dropped != 0)).astype(jnp.int32)
    return inside[:, None] * inside[None, :]


def levels(own_key, extent, split, least, largest):
    loudness, own = 1.0, jax.random.fold_in(own_key, 6)
    for axis_at, shards_of in split:
        steps = jnp.exp(jax.random.uniform(jax.random.fold_in(own, axis_at), (shards_of,), jnp.float32, least / len(split), largest / len(split)))
        loudness = loudness * jnp.repeat(steps, extent[axis_at] // shards_of).reshape([-1 if axis == axis_at else 1 for axis in range(len(extent))])
    return loudness


def bell_draw(stream_key, shape, width, most, cuts=(), kind=jnp.bfloat16):
    factor_of = levels(stream_key, shape, cuts, -0.22, 0.18) if cuts else 1.0
    result = jax.random.normal(stream_key, shape, jnp.float32) * width * factor_of
    return jnp.minimum(jnp.maximum(result, -most), most).astype(kind)


def setup_inputs(seed: int = 0) -> dict:
    seeds = jax.random.split(jax.random.key(seed), 8)
    pair = bell_draw(seeds[0], (C, N, N), 1.0, 6.0, ((0, 4), (1, 4), (2, 2)))
    pair_mask = draw_pair_mask(jax.random.fold_in(seeds[7], 71), 0)
    input_gain = jnp.clip(1.0 + 0.18 * jax.random.normal(seeds[2], (C,), jnp.float32), 0.1, 1.9)
    input_weights = bell_draw(seeds[3], (4, C, CH), C ** -0.5, 0.5)
    out_gate_weight = bell_draw(seeds[4], (C, C), C ** -0.5, 0.5)
    hidden_gain = jnp.clip(1.0 + 0.18 * jax.random.normal(seeds[5], (CH,), jnp.float32), 0.1, 1.9)
    out_weight = bell_draw(seeds[6], (CH, C), CH ** -0.5, 0.5)
    return dict(pair=pair, pair_mask=pair_mask, input_gain=input_gain, input_weights=input_weights, out_gate_weight=out_gate_weight, hidden_gain=hidden_gain, out_weight=out_weight)


EPSILON = 1e-05

def layer_norm(values, gains):
    average = lax.optimization_barrier(jnp.mean(values, axis=0))
    spread = lax.optimization_barrier(jnp.mean(jnp.square(values - average), axis=0))
    return (values - average) * lax.rsqrt(spread + EPSILON) * gains[:, None, None]

def project(weights, normed):
    return jnp.einsum('dk,drs->krs', weights.astype(jnp.float32), normed.astype(jnp.float32))

def reference(pair, pair_mask, input_gain, input_weights, out_gate_weight, hidden_gain, out_weight):
    normed = layer_norm(pair.astype(jnp.float32), input_gain).astype(jnp.bfloat16)
    mask_values = pair_mask.astype(jnp.float32)
    left_side = (mask_values * jax.nn.sigmoid(project(input_weights[0], normed)) * project(input_weights[1], normed)).astype(jnp.bfloat16)
    right_side = (mask_values * jax.nn.sigmoid(project(input_weights[2], normed)) * project(input_weights[3], normed)).astype(jnp.bfloat16)
    gate = jax.nn.sigmoid(project(out_gate_weight, normed))
    triangle = jnp.einsum('hki,hkj->hij', left_side.astype(jnp.float32), right_side.astype(jnp.float32))
    hidden_normed = layer_norm(triangle, hidden_gain).astype(jnp.bfloat16)
    projected = project(out_weight, hidden_normed)
    return (mask_values * gate * projected).astype(jnp.bfloat16)
```

```python
import jax
import jax.numpy as jnp
from jax import lax
from jax.sharding import PartitionSpec as P

EPSILON = 1e-05


def block_order(own, count, width):
    blocks = own ^ jnp.arange(count)
    return (blocks[:, None] * width + jnp.arange(width)[None, :]).reshape(-1)


def take_exact(order, matrix, axis):
    size = matrix.shape[axis]
    hot = (order[:, None] == jnp.arange(size)[None, :]).astype(matrix.dtype)
    moved = jnp.moveaxis(matrix, axis, -1)
    out = jnp.einsum("...c,ac->...a", moved, hot, preferred_element_type=jnp.float32)
    return jnp.moveaxis(out.astype(matrix.dtype), -1, axis)


def take_vector(order, vector):
    hot = order[:, None] == jnp.arange(vector.shape[0])[None, :]
    return jnp.sum(jnp.where(hot, vector[None, :], 0.0), axis=1)


def shards(pair, pair_mask, input_gain, input_weights, out_gate_weight, hidden_gain, out_weight):
    bf16, f32 = jnp.bfloat16, jnp.float32
    local_channels, rows, columns = pair.shape
    channels, hidden = input_gain.shape[0], hidden_gain.shape[0]
    depth, planes = lax.axis_size("gx"), lax.axis_size("gz")
    half_depth = depth // 2
    group = half_depth * planes
    sub_rows = rows // planes
    sub_hidden = hidden // group
    z, core, g = lax.axis_index("gx"), lax.axis_index("gy"), lax.axis_index("gz")
    half, inner = z // half_depth, z % half_depth
    place = inner * planes + g

    def across_gz(block, m):
        return lax.ppermute(block, "gz", [(i, i ^ m) for i in range(planes)])

    def across_group(block, m):
        pairs = []
        for a in range(depth):
            for b in range(planes):
                to = (a % half_depth * planes + b) ^ m
                pairs.append((a * planes + b, (a // half_depth * half_depth + to // planes) * planes + to % planes))
        return lax.ppermute(block, ("gx", "gz"), pairs)

    by_row = jnp.transpose(pair, (1, 0, 2))
    row_block = lambda m: lax.dynamic_slice_in_dim(by_row, (g ^ m) * sub_rows, sub_rows, 0)
    received = [across_gz(row_block(m), m) if m else row_block(0) for m in range(planes)]
    channel_order = block_order(g, planes, local_channels)
    hidden_order = block_order(place, group, sub_hidden)
    gains = take_vector(channel_order, input_gain)
    values = jnp.concatenate(received, axis=1).astype(f32)
    centred = values - jnp.mean(values, axis=1, keepdims=True)
    spread = jnp.mean(centred * centred, axis=1, keepdims=True)
    normed = (centred * lax.rsqrt(spread + EPSILON) * gains[None, :, None]).astype(bf16)
    own_mask = lax.dynamic_slice_in_dim(pair_mask, g * sub_rows, sub_rows, 0).astype(f32)

    weights = take_exact(hidden_order, take_exact(channel_order, input_weights, 1), 2)
    gates, sides = (
        jnp.concatenate(
            [weights[a].reshape(channels, group, 1, sub_hidden), weights[a + 2].reshape(channels, group, 1, sub_hidden)], 2
        ).reshape(channels, 2 * hidden)
        for a in (0, 1)
    )
    product = lambda w: jnp.einsum("ck,rcs->krs", w, normed, preferred_element_type=f32)
    both = (own_mask[None] * jax.nn.sigmoid(product(gates)) * product(sides)).astype(bf16)
    both = both.reshape(group, 2, sub_hidden, sub_rows, columns)
    collected = [across_group(both[m], m) if m else both[0] for m in range(group)]
    left = jnp.concatenate([b[0] for b in collected], axis=1)
    right = jnp.concatenate([b[1] for b in collected], axis=1)
    other_left = lax.ppermute(left, "gy", [(0, 1), (1, 0)])
    mine = core == half
    near = jnp.where(mine, left, other_left)
    far = jnp.where(mine, other_left, left)
    partial = lambda l: jnp.einsum("hki,hkj->hij", l, right, preferred_element_type=f32)
    sent = partial(far).astype(bf16)
    arrived = lax.ppermute(sent, "gx", [(i, (i + half_depth) % depth) for i in range(depth)])
    triangle = (partial(near) + arrived.astype(f32)).astype(bf16)
    tri_block = lambda m: lax.dynamic_slice_in_dim(triangle, (place ^ m) * sub_rows, sub_rows, 1)
    parts = [across_group(tri_block(m), m) if m else tri_block(0) for m in range(group)]
    hidden_values = jnp.concatenate(parts, axis=0).astype(f32)
    hidden_centred = hidden_values - jnp.mean(hidden_values, axis=0)
    hidden_spread = jnp.mean(hidden_centred * hidden_centred, axis=0)
    hidden_gains = take_vector(hidden_order, hidden_gain)
    hidden_normed = (hidden_centred * lax.rsqrt(hidden_spread + EPSILON) * hidden_gains[:, None, None]).astype(bf16)
    projection = take_exact(hidden_order, take_exact(channel_order, out_weight, 1), 0)
    gate_weights = take_exact(channel_order, take_exact(channel_order, out_gate_weight, 0), 1)
    gate = jax.nn.sigmoid(jnp.einsum("dc,rds->rcs", gate_weights, normed, preferred_element_type=f32))
    projected = jnp.einsum("hc,hrs->rcs", projection, hidden_normed, preferred_element_type=f32)
    update = (own_mask[:, None, :] * gate * projected).astype(bf16)
    out = jnp.zeros((rows, local_channels, columns), bf16)
    for m in range(planes):
        block = update[:, m * local_channels : (m + 1) * local_channels]
        block = across_gz(block, m) if m else block
        out = lax.dynamic_update_slice_in_dim(out, block, (g ^ m) * sub_rows, 0)
    return jnp.transpose(out, (1, 0, 2))


def solution(mesh):
    placed = (P("gz", "gx", "gy"), P("gx", "gy"), P(), P(), P(), P(), P())
    return jax.shard_map(
        shards, mesh=mesh, in_specs=placed, out_specs=P("gz", "gx", "gy"), check_vma=False
    )
```

```python
import jax
import jax.numpy as jnp
from jax import lax
from jax.sharding import PartitionSpec as P

EPSILON = 1e-05


def block_order(own, count, width, first, size):
    blocks = own ^ jnp.arange(count)
    return (blocks[:, None] * width + first + jnp.arange(size)[None, :]).reshape(-1)


def take_exact(order, matrix, axis):
    size = matrix.shape[axis]
    hot = (order[:, None] == jnp.arange(size)[None, :]).astype(matrix.dtype)
    moved = jnp.moveaxis(matrix, axis, -1)
    out = jnp.einsum("...c,ac->...a", moved, hot, preferred_element_type=jnp.float32)
    return jnp.moveaxis(out.astype(matrix.dtype), -1, axis)


def take_vector(order, vector):
    hot = order[:, None] == jnp.arange(vector.shape[0])[None, :]
    return jnp.sum(jnp.where(hot, vector[None, :], 0.0), axis=1)


def cuts(size):
    if size % 4:
        return [(0, size, 1)]
    q = size // 4
    return [(0, q, 1), (q, q, 1), (2 * q, 2 * q, 2)]


def shards(pair, pair_mask, input_gain, input_weights, out_gate_weight, hidden_gain, out_weight):
    bf16, f32 = jnp.bfloat16, jnp.float32
    local_channels, rows, columns = pair.shape
    channels, hidden = input_gain.shape[0], hidden_gain.shape[0]
    depth, planes = lax.axis_size("gx"), lax.axis_size("gz")
    half_depth = depth // 2
    group = half_depth * planes
    sub_rows = rows // planes
    sub_hidden = hidden // group
    z, core, g = lax.axis_index("gx"), lax.axis_index("gy"), lax.axis_index("gz")
    half, inner = z // half_depth, z % half_depth
    place = inner * planes + g
    chunks = cuts(sub_hidden)
    pieces = max(c[2] for c in chunks)

    def across_gz(block, m):
        return lax.ppermute(block, "gz", [(i, i ^ m) for i in range(planes)]) if m else block

    def across_group(block, m):
        if not m:
            return block
        pairs = []
        for a in range(depth):
            for b in range(planes):
                to = (a % half_depth * planes + b) ^ m
                pairs.append((a * planes + b, (a // half_depth * half_depth + to // planes) * planes + to % planes))
        return lax.ppermute(block, ("gx", "gz"), pairs)

    by_row = jnp.transpose(pair, (1, 0, 2))
    row_block = lambda m: lax.dynamic_slice_in_dim(by_row, (g ^ m) * sub_rows, sub_rows, 0)
    received = [across_gz(row_block(m), m) for m in range(planes)]
    channel_order = block_order(g, planes, local_channels, 0, local_channels)
    gains = take_vector(channel_order, input_gain)
    values = jnp.concatenate(received, axis=1).astype(f32)
    centred = values - jnp.mean(values, axis=1, keepdims=True)
    spread = jnp.mean(centred * centred, axis=1, keepdims=True)
    normed = (centred * lax.rsqrt(spread + EPSILON) * gains[None, :, None]).astype(bf16)
    own_mask = lax.dynamic_slice_in_dim(pair_mask, g * sub_rows, sub_rows, 0).astype(f32)
    own_weights = take_exact(channel_order, input_weights, 1)
    mine = core == half
    turned = normed
    parts = [[] for _ in range(pieces)]
    orders = []
    for first, size, split in chunks:
        order = block_order(place, group, sub_hidden, first, size)
        orders.append(order)
        weights = take_exact(order, own_weights, 2)
        gates, sides = (
            jnp.concatenate(
                [weights[a].reshape(channels, group, 1, size), weights[a + 2].reshape(channels, group, 1, size)], 2
            ).reshape(channels, 2 * group * size)
            for a in (0, 1)
        )
        product = lambda w: jnp.einsum("ck,rcs->krs", w, turned, preferred_element_type=f32)
        both = (own_mask[None] * jax.nn.sigmoid(product(gates)) * product(sides)).astype(bf16)
        both = both.reshape(group, 2, size, sub_rows, columns)
        turned, both = lax.optimization_barrier((turned, both))
        collected = [across_group(both[m], m) for m in range(group)]
        left = jnp.concatenate([b[0] for b in collected], axis=1)
        right = jnp.concatenate([b[1] for b in collected], axis=1)
        other_left = lax.ppermute(left, "gy", [(0, 1), (1, 0)])
        near = jnp.where(mine, left, other_left)
        far = jnp.where(mine, other_left, left)
        width = columns // split
        for at in range(split):
            piece = right[:, :, at * width : (at + 1) * width]
            partial = lambda l: jnp.einsum("hki,hkj->hij", l, piece, preferred_element_type=f32)
            sent = partial(far).astype(bf16)
            arrived = lax.ppermute(sent, "gx", [(i, (i + half_depth) % depth) for i in range(depth)])
            triangle = (partial(near) + arrived.astype(f32)).astype(bf16)
            tri_block = lambda m: lax.dynamic_slice_in_dim(triangle, (place ^ m) * sub_rows, sub_rows, 1)
            got = jnp.concatenate([across_group(tri_block(m), m) for m in range(group)], axis=0)
            share = pieces // split
            for sub in range(share):
                step = width // share
                parts[at * share + sub].append(got[:, :, sub * step : (sub + 1) * step])
    hidden_order = jnp.concatenate(orders)
    hidden_gains = take_vector(hidden_order, hidden_gain)
    projection = take_exact(hidden_order, take_exact(channel_order, out_weight, 1), 0)
    gate_weights = take_exact(channel_order, take_exact(channel_order, out_gate_weight, 0), 1)
    gate = jax.nn.sigmoid(jnp.einsum("dc,rds->rcs", gate_weights, turned, preferred_element_type=f32))
    gate = own_mask[:, None, :] * gate
    out = jnp.zeros((rows, local_channels, columns), bf16)
    step = columns // pieces
    for at in range(pieces):
        hidden_values = jnp.concatenate(parts[at], axis=0).astype(f32)
        hidden_centred = hidden_values - jnp.mean(hidden_values, axis=0)
        hidden_spread = jnp.mean(hidden_centred * hidden_centred, axis=0)
        hidden_normed = (
            hidden_centred * lax.rsqrt(hidden_spread + EPSILON) * hidden_gains[:, None, None]
        ).astype(bf16)
        projected = jnp.einsum("hc,hrs->rcs", projection, hidden_normed, preferred_element_type=f32)
        update = (gate[:, :, at * step : (at + 1) * step] * projected).astype(bf16)
        for m in range(planes):
            block = across_gz(update[:, m * local_channels : (m + 1) * local_channels], m)
            out = lax.dynamic_update_slice(out, block, ((g ^ m) * sub_rows, 0, at * step))
    return jnp.transpose(out, (1, 0, 2))


def solution(mesh):
    placed = (P("gz", "gx", "gy"), P("gx", "gy"), P(), P(), P(), P(), P())
    return jax.shard_map(
        shards, mesh=mesh, in_specs=placed, out_specs=P("gz", "gx", "gy"), check_vma=False
    )
```

```python
import jax
import jax.numpy as jnp
from jax import lax
from jax.sharding import PartitionSpec as P

EPSILON = 1e-05


def block_order(own, count, width, first, size):
    blocks = own ^ jnp.arange(count)
    return (blocks[:, None] * width + first + jnp.arange(size)[None, :]).reshape(-1)


def take_exact(order, matrix, axis):
    size = matrix.shape[axis]
    hot = (order[:, None] == jnp.arange(size)[None, :]).astype(matrix.dtype)
    moved = jnp.moveaxis(matrix, axis, -1)
    out = jnp.einsum("...c,ac->...a", moved, hot, preferred_element_type=jnp.float32)
    return jnp.moveaxis(out.astype(matrix.dtype), -1, axis)


def take_vector(order, vector):
    hot = order[:, None] == jnp.arange(vector.shape[0])[None, :]
    return jnp.sum(jnp.where(hot, vector[None, :], 0.0), axis=1)


def after(value, *others):
    return lax.optimization_barrier((value, *others))[0]


def shards(pair, pair_mask, input_gain, input_weights, out_gate_weight, hidden_gain, out_weight):
    bf16, f32 = jnp.bfloat16, jnp.float32
    local_channels, rows, columns = pair.shape
    channels, hidden = input_gain.shape[0], hidden_gain.shape[0]
    depth, planes = lax.axis_size("gx"), lax.axis_size("gz")
    half_depth = depth // 2
    group = half_depth * planes
    sub_rows = rows // planes
    sub_hidden = hidden // group
    z, core, g = lax.axis_index("gx"), lax.axis_index("gy"), lax.axis_index("gz")
    half, inner = z // half_depth, z % half_depth
    place = inner * planes + g
    chunks = [(0, sub_hidden // 2, 1), (sub_hidden // 2, sub_hidden // 2, 2)]
    pieces = 2

    def across_gz(block, m):
        return lax.ppermute(block, "gz", [(i, i ^ m) for i in range(planes)]) if m else block

    def across_group(block, m):
        if not m:
            return block
        pairs = []
        for a in range(depth):
            for b in range(planes):
                to = (a % half_depth * planes + b) ^ m
                pairs.append((a * planes + b, (a // half_depth * half_depth + to // planes) * planes + to % planes))
        return lax.ppermute(block, ("gx", "gz"), pairs)

    def across_halves(block):
        return lax.ppermute(block, "gx", [(i, (i + half_depth) % depth) for i in range(depth)])

    by_row = jnp.transpose(pair, (1, 0, 2))
    row_block = lambda m: lax.dynamic_slice_in_dim(by_row, (g ^ m) * sub_rows, sub_rows, 0)
    received = [across_gz(row_block(m), m) for m in range(planes)]
    channel_order = block_order(g, planes, local_channels, 0, local_channels)
    gains = take_vector(channel_order, input_gain)
    values = jnp.concatenate(received, axis=1).astype(f32)
    centred = values - jnp.mean(values, axis=1, keepdims=True)
    spread = jnp.mean(centred * centred, axis=1, keepdims=True)
    normed = (centred * lax.rsqrt(spread + EPSILON) * gains[None, :, None]).astype(bf16)
    own_mask = lax.dynamic_slice_in_dim(pair_mask, g * sub_rows, sub_rows, 0).astype(f32)
    own_weights = take_exact(channel_order, input_weights, 1)
    mine = core == half
    hidden_order = jnp.concatenate([block_order(place, group, sub_hidden, first, size) for first, size, _ in chunks])
    hidden_gains = take_vector(hidden_order, hidden_gain)
    projection = take_exact(hidden_order, take_exact(channel_order, out_weight, 1), 0)
    gate_weights = take_exact(channel_order, take_exact(channel_order, out_gate_weight, 0), 1)
    turned = normed
    last_sent = None
    pending = []
    for first, size, split in chunks:
        order = block_order(place, group, sub_hidden, first, size)
        weights = take_exact(order, own_weights, 2)
        gates, sides = (
            jnp.concatenate(
                [weights[a].reshape(channels, group, 1, size), weights[a + 2].reshape(channels, group, 1, size)], 2
            ).reshape(channels, 2 * group * size)
            for a in (0, 1)
        )
        product = lambda w: jnp.einsum("ck,rcs->krs", w, turned, preferred_element_type=f32)
        both = (own_mask[None] * jax.nn.sigmoid(product(gates)) * product(sides)).astype(bf16)
        both = both.reshape(group, 2, size, sub_rows, columns)
        collected = [across_group(both[m], m) for m in range(group)]
        turned = after(turned, both)
        if last_sent is not None:
            collected = [after(c, last_sent) for c in collected]
        left = jnp.concatenate([b[0] for b in collected], axis=1)
        right = jnp.concatenate([b[1] for b in collected], axis=1)
        other_left = lax.ppermute(left, "gy", [(0, 1), (1, 0)])
        near = jnp.where(mine, left, other_left)
        far = jnp.where(mine, other_left, left)
        width = columns // split
        for at in range(split):
            piece = right[:, :, at * width : (at + 1) * width]
            partial = lambda l: jnp.einsum("hki,hkj->hij", l, piece, preferred_element_type=f32)
            sent = partial(far).astype(bf16)
            last_sent = sent
            arrived = across_halves(sent)
            kept = after(partial(near))
            pending.append((kept, arrived))

    def back(at, *earlier):
        kept, arrived = pending[at]
        triangle = (kept + after(arrived, last_sent, *earlier).astype(f32)).astype(bf16)
        tri_block = lambda m: lax.dynamic_slice_in_dim(triangle, (place ^ m) * sub_rows, sub_rows, 1)
        return [across_group(tri_block(m), m) for m in range(group)]

    gate = jax.nn.sigmoid(jnp.einsum("dc,rds->rcs", gate_weights, turned, preferred_element_type=f32))
    gate = own_mask[:, None, :] * gate
    step = columns // pieces
    first_back = back(0)
    update = None
    blocks = []
    for at in range(pieces):
        got = back(at + 1) if update is None else back(at + 1, update)
        got = [b[:, :, at * step : (at + 1) * step] for b in first_back] + got
        hidden_values = jnp.concatenate(got, axis=0).astype(f32)
        hidden_centred = hidden_values - jnp.mean(hidden_values, axis=0)
        hidden_spread = jnp.mean(hidden_centred * hidden_centred, axis=0)
        hidden_normed = (
            hidden_centred * lax.rsqrt(hidden_spread + EPSILON) * hidden_gains[:, None, None]
        ).astype(bf16)
        projected = jnp.einsum("hc,hrs->rcs", projection, hidden_normed, preferred_element_type=f32)
        update = (gate[:, :, at * step : (at + 1) * step] * projected).astype(bf16)
        blocks.append([across_gz(update[:, m * local_channels : (m + 1) * local_channels], m) for m in range(planes)])
    out = jnp.zeros((rows, local_channels, columns), bf16)
    for at in range(pieces):
        for m in range(planes):
            out = lax.dynamic_update_slice(out, blocks[at][m], ((g ^ m) * sub_rows, 0, at * step))
    return jnp.transpose(out, (1, 0, 2))


def solution(mesh):
    placed = (P("gz", "gx", "gy"), P("gx", "gy"), P(), P(), P(), P(), P())

    return jax.shard_map(shards, mesh=mesh, in_specs=placed, out_specs=P("gz", "gx", "gy"), check_vma=False)
```

```python
import jax
import jax.numpy as jnp
from jax import lax
from jax.sharding import PartitionSpec as P

EPSILON = 1e-05


def block_order(own, count, width, first, size):
    blocks = own ^ jnp.arange(count)
    return (blocks[:, None] * width + first + jnp.arange(size)[None, :]).reshape(-1)


def take_exact(order, matrix, axis):
    size = matrix.shape[axis]
    hot = (order[:, None] == jnp.arange(size)[None, :]).astype(matrix.dtype)
    moved = jnp.moveaxis(matrix, axis, -1)
    out = jnp.einsum("...c,ac->...a", moved, hot, preferred_element_type=jnp.float32)
    return jnp.moveaxis(out.astype(matrix.dtype), -1, axis)


def take_vector(order, vector):
    hot = order[:, None] == jnp.arange(vector.shape[0])[None, :]
    return jnp.sum(jnp.where(hot, vector[None, :], 0.0), axis=1)


def after(value, *others):
    return lax.optimization_barrier((value, *others))[0]


def shards(pair, pair_mask, input_gain, input_weights, out_gate_weight, hidden_gain, out_weight):
    bf16, f32 = jnp.bfloat16, jnp.float32
    local_channels, rows, columns = pair.shape
    channels, hidden = input_gain.shape[0], hidden_gain.shape[0]
    depth, planes = lax.axis_size("gx"), lax.axis_size("gz")
    half_depth = depth // 2
    group = half_depth * planes
    sub_rows = rows // planes
    sub_hidden = hidden // group
    z, core, g = lax.axis_index("gx"), lax.axis_index("gy"), lax.axis_index("gz")
    half = z // half_depth
    inner = jnp.where(half == 0, z, depth - 1 - z)
    place = inner * planes + g
    chunks = [(0, sub_hidden // 2, 1), (sub_hidden // 2, sub_hidden // 2, 2)]
    pieces = 2
    step = sub_rows // pieces

    def across_gz(block, m):
        return lax.ppermute(block, "gz", [(i, i ^ m) for i in range(planes)]) if m else block

    def across_group(block, m):
        if not m:
            return block
        pairs = []
        for a in range(half_depth):
            for b in range(planes):
                to, at = divmod((a * planes + b) ^ m, planes)
                pairs.append((a * planes + b, to * planes + at))
                pairs.append(((depth - 1 - a) * planes + b, (depth - 1 - to) * planes + at))
        return lax.ppermute(block, ("gx", "gz"), pairs)

    middle = (half_depth - 1, half_depth)

    outer = [i for i in range(depth) if i not in middle]

    def across_halves(block, whose):
        return lax.ppermute(block, "gx", [(i, depth - 1 - i) for i in whose])

    def to_plane(block, e, far):
        pairs = []
        for i in range(half_depth):
            to = i ^ e
            ends = ((i, depth - 1 - to), (depth - 1 - i, to)) if far else ((i, to), (depth - 1 - i, depth - 1 - to))
            pairs += ends
        return lax.ppermute(block, "gx", pairs)

    def level(which, index):
        return jnp.where(which == 0, index, half_depth - 1 - index)

    by_row = jnp.transpose(pair, (1, 0, 2))
    row_block = lambda m: lax.dynamic_slice_in_dim(by_row, (g ^ m) * sub_rows, sub_rows, 0)
    received = [across_gz(row_block(m), m) for m in range(planes)]
    channel_order = block_order(g, planes, local_channels, 0, local_channels)
    gains = take_vector(channel_order, input_gain)
    values = jnp.concatenate(received, axis=1).astype(f32)
    centred = values - jnp.mean(values, axis=1, keepdims=True)
    spread = jnp.mean(centred * centred, axis=1, keepdims=True)
    normed = (centred * lax.rsqrt(spread + EPSILON) * gains[None, :, None]).astype(bf16)
    own_mask = lax.dynamic_slice_in_dim(pair_mask, g * sub_rows, sub_rows, 0).astype(f32)
    own_weights = take_exact(channel_order, input_weights, 1)
    mine = core == half
    hidden_order = jnp.concatenate([block_order(place, group, sub_hidden, first, size) for first, size, _ in chunks])
    hidden_gains = take_vector(hidden_order, hidden_gain)
    projection = take_exact(hidden_order, take_exact(channel_order, out_weight, 1), 0)
    gate_weights = take_exact(channel_order, take_exact(channel_order, out_gate_weight, 0), 1)
    turned = after(normed, projection)
    last_sent = None
    pending = []
    for at_chunk, (first, size, split) in enumerate(chunks):
        order = block_order(place, group, sub_hidden, first, size)
        weights = take_exact(order, own_weights, 2)
        gates, sides = (
            jnp.concatenate(
                [weights[a].reshape(channels, group, 1, size), weights[a + 2].reshape(channels, group, 1, size)], 2
            ).reshape(channels, 2 * group * size)
            for a in (0, 1)
        )
        product = lambda w: jnp.einsum("ck,rcs->rks", w, turned, preferred_element_type=f32)
        both = (own_mask[:, None, :] * jax.nn.sigmoid(product(gates)) * product(sides)).astype(bf16)
        block_of = lambda m: both[:, m * 2 * size : (m + 1) * 2 * size]
        collected = [across_group(block_of(m), m) for m in range(group)]
        turned = after(turned, both)
        if last_sent is not None:
            collected = [after(c, last_sent, gate_weights) for c in collected]
        operands = jnp.concatenate(collected, axis=0)
        left, right = operands[:, :size], operands[:, size:]
        other_left = lax.ppermute(left, "gy", [(0, 1), (1, 0)])
        near = jnp.where(mine, left, other_left)
        far = jnp.where(mine, other_left, left)
        partial = lambda l: jnp.einsum("khi,khj->hij", l, right, preferred_element_type=f32)
        last_sent = partial(far).astype(bf16)
        kept = after(partial(near))
        if not at_chunk:
            from_middle = across_halves(last_sent, middle)
            from_outer = across_halves(last_sent, outer)
            pending.append([(kept, jnp.where(inner == half_depth - 1, from_middle, from_outer))])
            continue
        for at in range(split):
            height = sub_rows // split

            def share_of(sums, which):
                planewise = sums.reshape(size, half_depth, planes, sub_rows, columns)[:, :, :, at * height : (at + 1) * height]
                return lax.dynamic_index_in_dim(planewise, which, 1, False)

            sums = []
            for e in range(half_depth):
                arrived = to_plane(share_of(last_sent, level(1 - half, inner ^ e)), e, True)
                own = share_of(kept, level(half, inner ^ e))
                if e:
                    own = to_plane(own.astype(bf16), e, False)
                sums.append((own, arrived))
            pending.append(sums)

    def back(at, *earlier):
        triangle = jnp.stack(
            [
                (own.astype(f32) + after(arrived, last_sent, *earlier).astype(f32)).astype(bf16)
                for own, arrived in pending[at]
            ]
        )
        if at:
            tri_block = lambda m: lax.dynamic_index_in_dim(triangle, g ^ m, 2, False)
            got = [across_gz(tri_block(m), m) for m in range(planes)]
            return [block[e] for e in range(half_depth) for block in got]
        triangle = triangle.reshape(-1, half_depth, planes, sub_rows, columns)

        def far_block(m):
            to = place ^ m
            flat = triangle.reshape(-1, group, sub_rows, columns)
            return lax.dynamic_index_in_dim(flat, level(half, to // planes) * planes + to % planes, 1, False)

        return [across_group(far_block(m), m) for m in range(group)]

    gate = jax.nn.sigmoid(jnp.einsum("dc,rds->rcs", gate_weights, turned, preferred_element_type=f32))
    gate = own_mask[:, None, :] * gate
    first_back = back(0)
    blocks = []
    for at in range(pieces):
        got = back(at + 1)
        got = [b[:, at * step : (at + 1) * step] for b in first_back] + got
        hidden_values = jnp.concatenate(got, axis=0).astype(f32)
        hidden_centred = hidden_values - jnp.mean(hidden_values, axis=0)
        hidden_spread = jnp.mean(hidden_centred * hidden_centred, axis=0)
        hidden_normed = (
            hidden_centred * lax.rsqrt(hidden_spread + EPSILON) * hidden_gains[:, None, None]
        ).astype(bf16)
        projected = jnp.einsum("hc,hrs->rcs", projection, hidden_normed, preferred_element_type=f32)
        update = (gate[at * step : (at + 1) * step] * projected).astype(bf16)
        blocks.append([across_gz(update[:, m * local_channels : (m + 1) * local_channels], m) for m in range(planes)])
    out = jnp.zeros((rows, local_channels, columns), bf16)
    for at in range(pieces):
        for m in range(planes):
            out = lax.dynamic_update_slice(out, blocks[at][m], ((g ^ m) * sub_rows + at * step, 0, 0))
    return jnp.transpose(out, (1, 0, 2))


def solution(mesh):
    placed = (P("gz", "gx", "gy"), P("gx", "gy"), P(), P(), P(), P(), P())

    return jax.shard_map(shards, mesh=mesh, in_specs=placed, out_specs=P("gz", "gx", "gy"), check_vma=False)
```

```python
import jax
import jax.numpy as jnp
from jax import lax
from jax.experimental import pallas as pl
from jax.sharding import PartitionSpec as P

EPSILON = 1e-05


def block_order(own, count, width, first, size):
    blocks = own ^ jnp.arange(count)
    return (blocks[:, None] * width + first + jnp.arange(size)[None, :]).reshape(-1)


def take_exact(order, matrix, axis):
    size = matrix.shape[axis]
    hot = (order[:, None] == jnp.arange(size)[None, :]).astype(matrix.dtype)
    moved = jnp.moveaxis(matrix, axis, -1)
    out = jnp.einsum("...c,ac->...a", moved, hot, preferred_element_type=jnp.float32)
    return jnp.moveaxis(out.astype(matrix.dtype), -1, axis)


def take_vector(order, vector):
    hot = order[:, None] == jnp.arange(vector.shape[0])[None, :]
    return jnp.sum(jnp.where(hot, vector[None, :], 0.0), axis=1)


def norm_and_gate_kernel(count, *refs):
    blocks, (mask, gains, gates, sides, normed, *parts) = refs[:count], refs[count:]
    width = parts[0].shape[1]
    for r in range(mask.shape[0]):
        values = jnp.concatenate([block[r].astype(jnp.float32) for block in blocks], axis=0)
        centred = values - jnp.mean(values, axis=0, keepdims=True)
        spread = jnp.mean(centred * centred, axis=0, keepdims=True)
        rounded = (centred * lax.rsqrt(spread + EPSILON) * gains[...]).astype(jnp.bfloat16)
        normed[r] = rounded
        left = jnp.dot(gates[...], rounded, preferred_element_type=jnp.float32)
        right = jnp.dot(sides[...], rounded, preferred_element_type=jnp.float32)
        both = (mask[r : r + 1, :] * jax.nn.sigmoid(left) * right).astype(jnp.bfloat16)
        for at, part in enumerate(parts):
            part[r] = both[at * width : (at + 1) * width]


def norm_and_gate(blocks, mask, gains, gates, sides, count):
    rows, width, columns = blocks[0].shape
    channels, outputs = len(blocks) * width, gates.shape[0]
    some = min(rows, 8)
    tall = lambda n: pl.BlockSpec((some, n, columns), lambda i: (i, 0, 0))
    whole = lambda a: pl.BlockSpec(a.shape, lambda i: (0, 0))
    return pl.pallas_call(
        lambda *refs: norm_and_gate_kernel(len(blocks), *refs),
        grid=(rows // some,),
        in_specs=[tall(width)] * len(blocks)
        + [pl.BlockSpec((some, columns), lambda i: (i, 0)), whole(gains), whole(gates), whole(sides)],
        out_specs=[tall(channels)] + [tall(outputs // count)] * count,
        out_shape=[jax.ShapeDtypeStruct((rows, channels, columns), jnp.bfloat16)]
        + [jax.ShapeDtypeStruct((rows, outputs // count, columns), jnp.bfloat16)] * count,
        cost_estimate=pl.CostEstimate(
            flops=4 * rows * columns * channels * outputs,
            bytes_accessed=4 * rows * columns * (channels + outputs),
            transcendentals=2 * rows * columns * outputs,
        ),
        name="norm_and_gate",
    )(*blocks, mask, gains, gates, sides)


def after(value, *others):
    return lax.optimization_barrier((value, *others))[0]


def shards(pair, pair_mask, input_gain, input_weights, out_gate_weight, hidden_gain, out_weight):
    bf16, f32 = jnp.bfloat16, jnp.float32
    local_channels, rows, columns = pair.shape
    channels, hidden = input_gain.shape[0], hidden_gain.shape[0]
    depth, planes = lax.axis_size("gx"), lax.axis_size("gz")
    half_depth = depth // 2
    group = half_depth * planes
    sub_rows = rows // planes
    sub_hidden = hidden // group
    z, core, g = lax.axis_index("gx"), lax.axis_index("gy"), lax.axis_index("gz")
    half = z // half_depth
    inner = jnp.where(half == 0, z, depth - 1 - z)
    place = inner * planes + g
    chunks = [(0, sub_hidden // 2, 1), (sub_hidden // 2, sub_hidden // 2, 2)]
    pieces = 2
    step = sub_rows // pieces

    def across_gz(block, m):
        return lax.ppermute(block, "gz", [(i, i ^ m) for i in range(planes)]) if m else block

    def across_group(block, m):
        if not m:
            return block
        pairs = []
        for a in range(half_depth):
            for b in range(planes):
                to, at = divmod((a * planes + b) ^ m, planes)
                pairs.append((a * planes + b, to * planes + at))
                pairs.append(((depth - 1 - a) * planes + b, (depth - 1 - to) * planes + at))
        return lax.ppermute(block, ("gx", "gz"), pairs)

    middle = (half_depth - 1, half_depth)

    outer = [i for i in range(depth) if i not in middle]

    def across_halves(block, whose):
        return lax.ppermute(block, "gx", [(i, depth - 1 - i) for i in whose])

    def to_plane(block, e, far):
        pairs = []
        for i in range(half_depth):
            to = i ^ e
            ends = ((i, depth - 1 - to), (depth - 1 - i, to)) if far else ((i, to), (depth - 1 - i, depth - 1 - to))
            pairs += ends
        return lax.ppermute(block, "gx", pairs)

    def level(which, index):
        return jnp.where(which == 0, index, half_depth - 1 - index)

    received = [None] * planes
    block = None
    for m in range(planes - 1, -1, -1):
        start = (g ^ m) * sub_rows
        start = start if block is None else after(start, block)
        block = jnp.transpose(lax.dynamic_slice_in_dim(pair, start, sub_rows, 1), (1, 0, 2))
        received[m] = across_gz(block, m)
    channel_order = block_order(g, planes, local_channels, 0, local_channels)
    gains = take_vector(channel_order, input_gain)
    own_mask = lax.dynamic_slice_in_dim(pair_mask, g * sub_rows, sub_rows, 0).astype(f32)
    own_weights = take_exact(channel_order, input_weights, 1)
    mine = core == half
    hidden_order = jnp.concatenate([block_order(place, group, sub_hidden, first, size) for first, size, _ in chunks])
    hidden_gains = take_vector(hidden_order, hidden_gain)
    projection = take_exact(hidden_order, take_exact(channel_order, out_weight, 1), 0)
    gate_weights = take_exact(channel_order, take_exact(channel_order, out_gate_weight, 0), 1)
    turned = None
    last_sent = None
    pending = []
    for at_chunk, (first, size, split) in enumerate(chunks):
        order = block_order(place, group, sub_hidden, first, size)
        weights = take_exact(order, own_weights, 2)
        gates, sides = (
            jnp.concatenate(
                [weights[a].reshape(channels, group, 1, size), weights[a + 2].reshape(channels, group, 1, size)], 2
            ).reshape(channels, 2 * group * size)
            for a in (0, 1)
        )
        if turned is None:
            turned, *both = norm_and_gate(received, own_mask, gains[:, None], gates.T, sides.T, group)
            turned = after(turned, projection)
        else:
            product = lambda w: jnp.einsum("ck,rcs->rks", w, turned, preferred_element_type=f32)
            both = (own_mask[:, None, :] * jax.nn.sigmoid(product(gates)) * product(sides)).astype(bf16)
            both = [both[:, m * 2 * size : (m + 1) * 2 * size] for m in range(group)]
        collected = [across_group(both[m], m) for m in range(group)]
        turned = after(turned, *both)
        if last_sent is not None:
            collected = [after(c, last_sent, gate_weights) for c in collected]
        operands = jnp.concatenate(collected, axis=0)
        left, right = operands[:, :size], operands[:, size:]
        other_left = lax.ppermute(left, "gy", [(0, 1), (1, 0)])
        near = jnp.where(mine, left, other_left)
        far = jnp.where(mine, other_left, left)
        partial = lambda l: jnp.einsum("khi,khj->hij", l, right, preferred_element_type=f32)
        last_sent = partial(far).astype(bf16)
        kept = after(partial(near))
        if not at_chunk:
            from_middle = across_halves(last_sent, middle)
            from_outer = across_halves(last_sent, outer)
            pending.append([(kept, jnp.where(inner == half_depth - 1, from_middle, from_outer))])
            continue
        for at in range(split):
            height = sub_rows // split

            def share_of(sums, which):
                planewise = sums.reshape(size, half_depth, planes, sub_rows, columns)[:, :, :, at * height : (at + 1) * height]
                return lax.dynamic_index_in_dim(planewise, which, 1, False)

            sums = []
            for e in range(half_depth):
                arrived = to_plane(share_of(last_sent, level(1 - half, inner ^ e)), e, True)
                own = share_of(kept, level(half, inner ^ e))
                if e:
                    own = to_plane(own.astype(bf16), e, False)
                sums.append((own, arrived))
            pending.append(sums)

    def back(at, *earlier):
        triangle = jnp.stack(
            [
                (own.astype(f32) + after(arrived, last_sent, *earlier).astype(f32)).astype(bf16)
                for own, arrived in pending[at]
            ]
        )
        if at:
            tri_block = lambda m: lax.dynamic_index_in_dim(triangle, g ^ m, 2, False)
            got = [across_gz(tri_block(m), m) for m in range(planes)]
            return [block[e] for e in range(half_depth) for block in got]
        triangle = triangle.reshape(-1, half_depth, planes, sub_rows, columns)

        def far_block(m):
            to = place ^ m
            flat = triangle.reshape(-1, group, sub_rows, columns)
            return lax.dynamic_index_in_dim(flat, level(half, to // planes) * planes + to % planes, 1, False)

        return [across_group(far_block(m), m) for m in range(group)]

    gate = jax.nn.sigmoid(jnp.einsum("dc,rds->rcs", gate_weights, turned, preferred_element_type=f32))
    gate = own_mask[:, None, :] * gate
    first_back = back(0)
    blocks = []
    for at in range(pieces):
        got = back(at + 1)
        got = [b[:, at * step : (at + 1) * step] for b in first_back] + got
        hidden_values = jnp.concatenate(got, axis=0).astype(f32)
        hidden_centred = hidden_values - jnp.mean(hidden_values, axis=0)
        hidden_spread = jnp.mean(hidden_centred * hidden_centred, axis=0)
        hidden_normed = (
            hidden_centred * lax.rsqrt(hidden_spread + EPSILON) * hidden_gains[:, None, None]
        ).astype(bf16)
        projected = jnp.einsum("hc,hrs->rcs", projection, hidden_normed, preferred_element_type=f32)
        update = (gate[at * step : (at + 1) * step] * projected).astype(bf16)
        blocks.append([across_gz(update[:, m * local_channels : (m + 1) * local_channels], m) for m in range(planes)])
    out = jnp.zeros((rows, local_channels, columns), bf16)
    for at in range(pieces):
        for m in range(planes):
            out = lax.dynamic_update_slice(out, blocks[at][m], ((g ^ m) * sub_rows + at * step, 0, 0))
    return jnp.transpose(out, (1, 0, 2))


def solution(mesh):
    placed = (P("gz", "gx", "gy"), P("gx", "gy"), P(), P(), P(), P(), P())

    return jax.shard_map(shards, mesh=mesh, in_specs=placed, out_specs=P("gz", "gx", "gy"), check_vma=False)
```

```python
import jax
import jax.numpy as jnp
from jax import lax
from jax.experimental import pallas as pl
from jax.sharding import PartitionSpec as P

EPSILON = 1e-05


def block_order(own, count, width, first, size):
    blocks = own ^ jnp.arange(count)
    return (blocks[:, None] * width + first + jnp.arange(size)[None, :]).reshape(-1)


def take_exact(order, matrix, axis):
    size = matrix.shape[axis]
    hot = (order[:, None] == jnp.arange(size)[None, :]).astype(matrix.dtype)
    moved = jnp.moveaxis(matrix, axis, -1)
    out = jnp.einsum("...c,ac->...a", moved, hot, preferred_element_type=jnp.float32)
    return jnp.moveaxis(out.astype(matrix.dtype), -1, axis)


def take_vector(order, vector):
    hot = order[:, None] == jnp.arange(vector.shape[0])[None, :]
    return jnp.sum(jnp.where(hot, vector[None, :], 0.0), axis=1)


def norm_and_gate_kernel(count, *refs):
    blocks, (mask, gains, gates, sides, normed, *parts) = refs[:count], refs[count:]
    width = parts[0].shape[1]
    for r in range(mask.shape[0]):
        values = jnp.concatenate([block[r].astype(jnp.float32) for block in blocks], axis=0)
        centred = values - jnp.mean(values, axis=0, keepdims=True)
        spread = jnp.mean(centred * centred, axis=0, keepdims=True)
        rounded = (centred * lax.rsqrt(spread + EPSILON) * gains[...]).astype(jnp.bfloat16)
        normed[r] = rounded
        left = jnp.dot(gates[...], rounded, preferred_element_type=jnp.float32)
        right = jnp.dot(sides[...], rounded, preferred_element_type=jnp.float32)
        both = (mask[r : r + 1, :] * jax.nn.sigmoid(left) * right).astype(jnp.bfloat16)
        for at, part in enumerate(parts):
            part[r] = both[at * width : (at + 1) * width]


def norm_and_gate(blocks, mask, gains, gates, sides, count):
    rows, width, columns = blocks[0].shape
    channels, outputs = len(blocks) * width, gates.shape[0]
    some = min(rows, 16)
    tall = lambda n: pl.BlockSpec((some, n, columns), lambda i: (i, 0, 0))
    whole = lambda a: pl.BlockSpec(a.shape, lambda i: (0, 0))
    return pl.pallas_call(
        lambda *refs: norm_and_gate_kernel(len(blocks), *refs),
        grid=(rows // some,),
        in_specs=[tall(width)] * len(blocks)
        + [pl.BlockSpec((some, columns), lambda i: (i, 0)), whole(gains), whole(gates), whole(sides)],
        out_specs=[tall(channels)] + [tall(outputs // count)] * count,
        out_shape=[jax.ShapeDtypeStruct((rows, channels, columns), jnp.bfloat16)]
        + [jax.ShapeDtypeStruct((rows, outputs // count, columns), jnp.bfloat16)] * count,
        cost_estimate=pl.CostEstimate(
            flops=4 * rows * columns * channels * outputs,
            bytes_accessed=4 * rows * columns * (channels + outputs),
            transcendentals=2 * rows * columns * outputs,
        ),
        name="norm_and_gate",
    )(*blocks, mask, gains, gates, sides)


def after(value, *others):
    return lax.optimization_barrier((value, *others))[0]


def shards(pair, pair_mask, input_gain, input_weights, out_gate_weight, hidden_gain, out_weight):
    bf16, f32 = jnp.bfloat16, jnp.float32
    local_channels, rows, columns = pair.shape
    channels, hidden = input_gain.shape[0], hidden_gain.shape[0]
    depth, planes = lax.axis_size("gx"), lax.axis_size("gz")
    half_depth = depth // 2
    group = half_depth * planes
    sub_rows = rows // planes
    sub_hidden = hidden // group
    z, core, g = lax.axis_index("gx"), lax.axis_index("gy"), lax.axis_index("gz")
    half = z // half_depth
    inner = jnp.where(half == 0, z, depth - 1 - z)
    place = inner * planes + g
    chunks = [(0, sub_hidden // 2, 1), (sub_hidden // 2, sub_hidden // 2, 2)]
    pieces = 2
    step = sub_rows // pieces

    def across_gz(block, m):
        return lax.ppermute(block, "gz", [(i, i ^ m) for i in range(planes)]) if m else block

    def across_group(block, m):
        if not m:
            return block
        pairs = []
        for a in range(half_depth):
            for b in range(planes):
                to, at = divmod((a * planes + b) ^ m, planes)
                pairs.append((a * planes + b, to * planes + at))
                pairs.append(((depth - 1 - a) * planes + b, (depth - 1 - to) * planes + at))
        return lax.ppermute(block, ("gx", "gz"), pairs)

    middle = (half_depth - 1, half_depth)

    outer = [i for i in range(depth) if i not in middle]

    def across_halves(block, whose):
        return lax.ppermute(block, "gx", [(i, depth - 1 - i) for i in whose])

    def to_plane(block, e, far):
        pairs = []
        for i in range(half_depth):
            to = i ^ e
            ends = ((i, depth - 1 - to), (depth - 1 - i, to)) if far else ((i, to), (depth - 1 - i, depth - 1 - to))
            pairs += ends
        return lax.ppermute(block, "gx", pairs)

    def level(which, index):
        return jnp.where(which == 0, index, half_depth - 1 - index)

    received = [None] * planes
    block = None
    for m in range(planes - 1, -1, -1):
        start = (g ^ m) * sub_rows
        start = start if block is None else after(start, block)
        block = jnp.transpose(lax.dynamic_slice_in_dim(pair, start, sub_rows, 1), (1, 0, 2))
        received[m] = across_gz(block, m)
    channel_order = block_order(g, planes, local_channels, 0, local_channels)
    gains = take_vector(channel_order, input_gain)
    own_mask = lax.dynamic_slice_in_dim(pair_mask, g * sub_rows, sub_rows, 0).astype(f32)
    own_weights = take_exact(channel_order, input_weights, 1)
    mine = core == half
    hidden_order = jnp.concatenate([block_order(place, group, sub_hidden, first, size) for first, size, _ in chunks])
    hidden_gains = take_vector(hidden_order, hidden_gain)
    projection = take_exact(hidden_order, take_exact(channel_order, out_weight, 1), 0)
    gate_weights = take_exact(channel_order, take_exact(channel_order, out_gate_weight, 0), 1)
    turned = None
    last_sent = None
    pending = []
    for at_chunk, (first, size, split) in enumerate(chunks):
        order = block_order(place, group, sub_hidden, first, size)
        weights = take_exact(order, own_weights, 2)
        gates, sides = (
            jnp.concatenate(
                [weights[a].reshape(channels, group, 1, size), weights[a + 2].reshape(channels, group, 1, size)], 2
            ).reshape(channels, 2 * group * size)
            for a in (0, 1)
        )
        if turned is None:
            turned, *both = norm_and_gate(received, own_mask, gains[:, None], gates.T, sides.T, group)
            turned = after(turned, projection)
        else:
            product = lambda w: jnp.einsum("ck,rcs->rks", w, turned, preferred_element_type=f32)
            both = (own_mask[:, None, :] * jax.nn.sigmoid(product(gates)) * product(sides)).astype(bf16)
            both = [both[:, m * 2 * size : (m + 1) * 2 * size] for m in range(group)]
        collected = [across_group(both[m], m) for m in range(group)]
        turned = after(turned, *both)
        if last_sent is not None:
            collected = [after(c, last_sent, gate_weights) for c in collected]
        operands = jnp.concatenate(collected, axis=0)
        left, right = operands[:, :size], operands[:, size:]
        other_left = lax.ppermute(left, "gy", [(0, 1), (1, 0)])
        near = jnp.where(mine, left, other_left)
        far = jnp.where(mine, other_left, left)
        partial = lambda l: jnp.einsum("khi,khj->hij", l, right, preferred_element_type=f32)
        last_sent = partial(far).astype(bf16)
        kept = after(partial(near))
        if not at_chunk:
            from_middle = across_halves(last_sent, middle)
            from_outer = across_halves(last_sent, outer)
            pending.append([(kept, jnp.where(inner == half_depth - 1, from_middle, from_outer))])
            continue
        for at in range(split):
            height = sub_rows // split

            def share_of(sums, which):
                planewise = sums.reshape(size, half_depth, planes, sub_rows, columns)[:, :, :, at * height : (at + 1) * height]
                return lax.dynamic_index_in_dim(planewise, which, 1, False)

            sums = []
            for e in range(half_depth):
                arrived = to_plane(share_of(last_sent, level(1 - half, inner ^ e)), e, True)
                own = share_of(kept, level(half, inner ^ e))
                if e:
                    own = to_plane(own.astype(bf16), e, False)
                sums.append((own, arrived))
            pending.append(sums)

    def back(at, *earlier):
        triangle = jnp.stack(
            [
                (own.astype(f32) + after(arrived, last_sent, *earlier).astype(f32)).astype(bf16)
                for own, arrived in pending[at]
            ]
        )
        if at:
            tri_block = lambda m: lax.dynamic_index_in_dim(triangle, g ^ m, 2, False)
            got = [across_gz(tri_block(m), m) for m in range(planes)]
            return [block[e] for e in range(half_depth) for block in got]
        triangle = triangle.reshape(-1, half_depth, planes, sub_rows, columns)

        def far_block(m):
            to = place ^ m
            flat = triangle.reshape(-1, group, sub_rows, columns)
            return lax.dynamic_index_in_dim(flat, level(half, to // planes) * planes + to % planes, 1, False)

        return [across_group(far_block(m), m) for m in range(group)]

    gate = jax.nn.sigmoid(jnp.einsum("dc,rds->rcs", gate_weights, turned, preferred_element_type=f32))
    gate = own_mask[:, None, :] * gate
    first_back = back(0)
    blocks = []
    for at in range(pieces):
        got = back(at + 1)
        got = [b[:, at * step : (at + 1) * step] for b in first_back] + got
        hidden_values = jnp.concatenate(got, axis=0).astype(f32)
        hidden_centred = hidden_values - jnp.mean(hidden_values, axis=0)
        hidden_spread = jnp.mean(hidden_centred * hidden_centred, axis=0)
        hidden_normed = (
            hidden_centred * lax.rsqrt(hidden_spread + EPSILON) * hidden_gains[:, None, None]
        ).astype(bf16)
        projected = jnp.einsum("hc,hrs->rcs", projection, hidden_normed, preferred_element_type=f32)
        update = (gate[at * step : (at + 1) * step] * projected).astype(bf16)
        blocks.append(
            [across_gz(update[:, m * local_channels : (m + 1) * local_channels], m) for m in reversed(range(planes))][::-1]
        )
    out = jnp.zeros((rows, local_channels, columns), bf16)
    for at in range(pieces):
        for m in range(planes):
            out = lax.dynamic_update_slice(out, blocks[at][m], ((g ^ m) * sub_rows + at * step, 0, 0))
    return jnp.transpose(out, (1, 0, 2))


def solution(mesh):
    placed = (P("gz", "gx", "gy"), P("gx", "gy"), P(), P(), P(), P(), P())

    return jax.shard_map(shards, mesh=mesh, in_specs=placed, out_specs=P("gz", "gx", "gy"), check_vma=False)
```
